256 devices in a mesh: ex: 16 (over y, x_lo, core), tp: 16 (over x_hi, z).
Axes of the slice: x: 4 (x_hi: 2, x_lo: 2; x = x_hi * 2 + x_lo), y: 4, z: 8, core: 2. Of those that a mesh axis runs over, the one named last changes fastest.
Arguments:
- samples: bfloat16 [1536, 2048], P(('ex', 'tp')), may hold values from -6 to 6
- gate_weight: bfloat16 [2048, 44], replicated, may hold values from -15 to 15
- up_weight: bfloat16 [16, 2048, 4096], P('ex', None, 'tp'), may hold values from -0.125 to 0.125
- down_weight: bfloat16 [16, 4096, 2048], P('ex', 'tp'), may hold values from -0.09375 to 0.09375
Outputs:
- task_outputs: bfloat16 [1536, 5, 2048], P(('ex', 'tp'))
The draws below stay inside these ranges and needn't reach their ends.
All inputs are finite; a program needn't handle non-finite values.
Results may differ from the reference program's by a relative error of at most 0.0055.
Values may be sent and summed in bfloat16 or wider, within the bound.
No kernel may reach another device: no remote copies, remote signals or barrier semaphores. Data moves between devices by JAX's collectives and lax.ppermute only.
A program may use at most 128 MiB of HBM per device.

```python
import jax
import jax.numpy as jnp
import numpy as np
from jax import lax

D = 2048
FF = 4096
TASKS = 4
TASK_EXP = 3
SHARED = 4
EXPERTS = 16
GATES = 44
ROWS = 1536


def draw_gate_weight(key, part):
    first_key = jax.random.fold_in(key, 11)
    base = jax.random.normal(first_key, (D, GATES), jnp.float32)
    values = base * (2.0 / jnp.sqrt(jnp.float32(D)))
    return jnp.clip(values, -15.0, 15.0).astype(jnp.bfloat16)


def levels(own_key, extent, shards, low, high):
    gain = 1.0
    for axis_at, shards_of in shards:
        heights = jax.random.uniform(jax.random.fold_in(jax.random.fold_in(own_key, 6), axis_at), (shards_of,), jnp.float32, low / len(shards), high / len(shards))
        gain = gain * jnp.repeat(jnp.exp(heights), extent[axis_at] // shards_of).reshape((-1,) + (1,) * (len(extent) - 1 - axis_at))
    return gain


def scatter_about(rng, extent, scale, limit, split=(), held_as=jnp.bfloat16):
    values = scale * jax.random.normal(rng, extent, jnp.float32)
    if split:
        values = values * levels(rng, extent, split, -0.22, 0.18)
    return jnp.clip(values, -limit, limit).astype(held_as)


def setup_inputs(seed: int = 0) -> dict:
    seeds = jax.random.split(jax.random.key(seed), 5)
    samples = scatter_about(seeds[0], (ROWS, D), 1.0, 6.0, ((0, 256),))
    gate_weight = draw_gate_weight(jax.random.fold_in(seeds[4], 71), 0)
    up_weight = scatter_about(seeds[2], (EXPERTS, D, FF), D ** -0.5, 0.125, ((0, 16), (2, 16)))
    down_weight = scatter_about(seeds[3], (EXPERTS, FF, D), FF ** -0.5, 0.09375, ((0, 16), (1, 16)))
    return dict(samples=samples, gate_weight=gate_weight, up_weight=up_weight, down_weight=down_weight)


def routing_table():
    per_task = TASK_EXP + SHARED
    table = np.zeros((GATES, (TASKS + 1) * EXPERTS), np.float32)
    for task_idx in range(TASKS):
        for column in range(per_task):
            if column < TASK_EXP:
                expert_idx = task_idx * TASK_EXP + column
            else:
                expert_idx = TASKS * TASK_EXP + column - TASK_EXP
            table[task_idx * per_task + column, task_idx * EXPERTS + expert_idx] = 1.0
    for expert_idx in range(EXPERTS):
        table[TASKS * per_task + expert_idx, TASKS * EXPERTS + expert_idx] = 1.0
    return jnp.asarray(table, dtype=jnp.float32)


def gate_mix(rows, gate_weight):
    logits = jnp.dot(rows, gate_weight, preferred_element_type=jnp.float32)
    per_task = TASK_EXP + SHARED
    pieces = []
    for task_idx in range(TASKS):
        pieces.append(jax.nn.softmax(logits[:, task_idx * per_task:(task_idx + 1) * per_task], axis=-1))
    pieces.append(jax.nn.softmax(logits[:, TASKS * per_task:], axis=-1))
    probs = jnp.concatenate(pieces, axis=1)
    mixed = jnp.dot(probs, routing_table(), precision=lax.Precision.HIGHEST)
    return mixed.reshape(rows.shape[0], TASKS + 1, EXPERTS)


def reference(samples, gate_weight, up_weight, down_weight):
    mixing = gate_mix(samples, gate_weight)
    weights_by_expert = jnp.transpose(mixing, (2, 0, 1))

    def accumulate(total, item):
        first, second, weighs = item
        hidden = jnp.maximum(jnp.dot(samples, first, preferred_element_type=jnp.float32), 0.0).astype(jnp.bfloat16)
        expert_out = jnp.dot(hidden, second, preferred_element_type=jnp.float32)
        return total + weighs[:, :, None] * expert_out[:, None, :], None

    start_total = jnp.zeros((samples.shape[0], TASKS + 1, samples.shape[1]), jnp.float32)
    total, unused = lax.scan(accumulate, start_total, (up_weight, down_weight, weights_by_expert))
    return total.astype(jnp.bfloat16)
```

```python
import functools

import jax
import jax.numpy as jnp
import numpy as np
from jax import lax
from jax.experimental import pallas as pl
from jax.experimental.pallas import tpu as pltpu
from jax.sharding import Mesh
from jax.sharding import PartitionSpec as P

TASKS = 4
TASK_EXP = 3
SHARED = 4
EXPERTS = 16
GATES = 44
AXES = ("y", "xl", "c", "xh", "z")
SIZES = (4, 2, 2, 2, 8)
NY, NXL, NC, NXH, NZ = SIZES


def shift(x, axis, by):
    n = lax.axis_size(axis)
    return lax.ppermute(x, axis, [(i, (i + by) % n) for i in range(n)])


def routing_table():
    per_task = TASK_EXP + SHARED
    table = np.zeros((GATES, (TASKS + 1) * EXPERTS), np.float32)
    for task_idx in range(TASKS):
        for column in range(per_task):
            if column < TASK_EXP:
                expert_idx = task_idx * TASK_EXP + column
            else:
                expert_idx = TASKS * TASK_EXP + column - TASK_EXP
            table[task_idx * per_task + column, task_idx * EXPERTS + expert_idx] = 1.0
    for expert_idx in range(EXPERTS):
        table[TASKS * per_task + expert_idx, TASKS * EXPERTS + expert_idx] = 1.0
    return jnp.asarray(table, dtype=jnp.float32)


def gate_mix(rows, gate_weight):
    logits = jnp.dot(rows, gate_weight, preferred_element_type=jnp.float32)
    per_task = TASK_EXP + SHARED
    pieces = []
    for task_idx in range(TASKS):
        pieces.append(
            jax.nn.softmax(logits[:, task_idx * per_task : (task_idx + 1) * per_task], axis=-1)
        )
    pieces.append(jax.nn.softmax(logits[:, TASKS * per_task :], axis=-1))
    probs = jnp.concatenate(pieces, axis=1)
    mixed = jnp.dot(probs, routing_table(), precision=lax.Precision.HIGHEST)
    return mixed.reshape(rows.shape[0], TASKS + 1, EXPERTS)


def row_order(rows):
    block = NXL * rows
    total = NY * NZ * block
    dest = lax.broadcasted_iota(jnp.int32, (total, total), 0)
    source = lax.broadcasted_iota(jnp.int32, (total, total), 1)
    k, rest = dest // (NY * block), dest % (NY * block)
    y, q = rest // block, rest % block
    dy = (lax.axis_index("y") - y + NY) % NY
    z = (lax.axis_index("z") + k) % NZ
    return (source == (dy * NZ + z) * block + q).astype(jnp.bfloat16)


def up_kernel(order_ref, *refs):
    samples, weights, out_ref = refs[:NY], refs[NY:-1], refs[-1]
    units = weights[0].shape[1]
    order = order_ref[...]
    for at, weight in enumerate(weights):
        hidden = jnp.concatenate(
            [
                jnp.maximum(
                    jnp.dot(piece[...], weight[...], preferred_element_type=jnp.float32), 0.0
                ).astype(jnp.bfloat16)
                for piece in samples
            ],
            axis=0,
        )
        out_ref[:, at * units : (at + 1) * units] = jnp.dot(
            order, hidden, preferred_element_type=jnp.float32
        ).astype(jnp.bfloat16)


def down_kernel(hidden_ref, *refs):
    weights, out_ref = refs[:-1], refs[-1]
    units, columns = weights[0].shape
    for expert in range(2):
        out_ref[:, expert * columns : (expert + 1) * columns] = jnp.dot(
            hidden_ref[:, 2 * expert * units : (2 * expert + 1) * units],
            weights[2 * expert][...],
            preferred_element_type=jnp.float32,
        ) + jnp.dot(
            hidden_ref[:, (2 * expert + 1) * units : (2 * expert + 2) * units],
            weights[2 * expert + 1][...],
            preferred_element_type=jnp.float32,
        )


def call(kernel, shape, dtype, flops, *args):
    vmem = pl.BlockSpec(memory_space=pltpu.VMEM)
    moved = sum(a.size * a.dtype.itemsize for a in args) + int(np.prod(shape)) * jnp.dtype(dtype).itemsize
    return pl.pallas_call(
        kernel,
        out_shape=jax.ShapeDtypeStruct(shape, dtype),
        in_specs=[vmem] * len(args),
        out_specs=vmem,
        cost_estimate=pl.CostEstimate(flops=flops, bytes_accessed=moved, transcendentals=0),
    )(*args)


def sum_along_z(parts, ahead, behind):
    low = lambda x: x.astype(jnp.bfloat16)
    up = low(parts[ahead])
    for k in range(ahead - 1, -1, -1):
        up = shift(up, "z", 1)
        if k:
            up = low(up.astype(jnp.float32) + parts[k])
    down = low(parts[NZ - behind])
    for k in range(NZ - behind + 1, NZ + 1):
        down = shift(down, "z", -1)
        if k < NZ:
            down = low(down.astype(jnp.float32) + parts[k])
    return low(parts[0] + up.astype(jnp.float32) + down.astype(jnp.float32))


def on_device(samples, gate_weight, up_weight, down_weight):
    rows, width = samples.shape
    up, down = up_weight[0], down_weight[0]
    units = up.shape[1]
    half = width // 2
    downs = (down[:, :half], down[:, half:])

    def spread(w):
        far = shift(w, "xh", 1)
        return [w, far, shift(w, "c", 1), shift(far, "c", 1)]

    ups = spread(up)
    down_halves = [spread(d) for d in downs]

    same = jnp.broadcast_to(samples[None], (NZ * NXL, rows, width))
    near = lax.all_to_all(same, ("z", "xl"), split_axis=0, concat_axis=0, tiled=True)
    near = near.reshape(NZ * NXL * rows, width)
    pieces = [near] + [shift(near, "y", dy) for dy in range(1, NY)]

    total = NY * NZ * NXL * rows
    hidden = call(
        up_kernel, (total, 4 * units), jnp.bfloat16, 2 * total * width * 4 * units,
        row_order(rows), *pieces, *ups,
    )
    summed = []
    for at, weights in enumerate(down_halves):
        partial = call(
            down_kernel, (total, 2 * half), jnp.float32, 2 * total * half * 4 * units,
            hidden, *weights,
        )
        chunk = total // NZ
        parts = [partial[k * chunk : (k + 1) * chunk] for k in range(NZ)]
        summed.append(sum_along_z(parts, *((4, 3) if at == 0 else (3, 4))))
    gathered = []
    for piece in summed:
        blocks = piece.reshape(NY * NXL, rows, 2 * half)
        moved = lax.all_to_all(blocks, ("y", "xl"), split_axis=0, concat_axis=0, tiled=True)
        gathered.append(moved.reshape(NY * NXL, rows, 2, half))

    mixing = gate_mix(samples, gate_weight).reshape(rows, TASKS + 1, NY * NXL, NC)
    own = lax.axis_index("c")
    mixing = jnp.where(own == 0, mixing, mixing[..., ::-1])
    out = [
        jnp.einsum("rkpj,prjd->krd", mixing, g.astype(jnp.float32), precision=lax.Precision.HIGHEST)
        for g in gathered
    ]
    return jnp.concatenate(out, axis=2).astype(jnp.bfloat16).transpose(1, 0, 2)


def solution(mesh):
    torus = Mesh(mesh.devices.reshape(SIZES), AXES)
    ex, tp = AXES[:3], AXES[3:]
    return jax.shard_map(
        on_device,
        mesh=torus,
        in_specs=(P(AXES, None), P(), P(ex, None, tp), P(ex, tp, None)),
        out_specs=P(AXES, None, None),
        check_vma=False,
    )
```

```python
import jax
import jax.numpy as jnp
import numpy as np
from jax import lax
from jax.experimental import pallas as pl
from jax.experimental.pallas import tpu as pltpu
from jax.sharding import Mesh
from jax.sharding import PartitionSpec as P


TASKS = 4
TASK_EXP = 3
SHARED = 4
EXPERTS = 16
GATES = 44
AXES = ("y", "xl", "c", "xh", "z")
SIZES = (4, 2, 2, 2, 8)
NY, NXL, NC, _, NZ = SIZES


def shift(x, axis, by):
    n = lax.axis_size(axis)
    return lax.ppermute(x, axis, [(i, (i + by) % n) for i in range(n)])


def routing_table():
    per_task = TASK_EXP + SHARED
    table = np.zeros((GATES, (TASKS + 1) * EXPERTS), np.float32)
    for task_idx in range(TASKS):
        for column in range(per_task):
            if column < TASK_EXP:
                expert_idx = task_idx * TASK_EXP + column
            else:
                expert_idx = TASKS * TASK_EXP + column - TASK_EXP
            table[task_idx * per_task + column, task_idx * EXPERTS + expert_idx] = 1.0
    for expert_idx in range(EXPERTS):
        table[TASKS * per_task + expert_idx, TASKS * EXPERTS + expert_idx] = 1.0
    return table


def gate_mix(rows, gate_weight):
    logits = jnp.dot(rows, gate_weight, preferred_element_type=jnp.float32)
    per_task = TASK_EXP + SHARED
    pieces = []
    for task_idx in range(TASKS):
        pieces.append(
            jax.nn.softmax(logits[:, task_idx * per_task : (task_idx + 1) * per_task], axis=-1)
        )
    pieces.append(jax.nn.softmax(logits[:, TASKS * per_task :], axis=-1))
    probs = jnp.concatenate(pieces, axis=1)
    table = routing_table()
    swapped = table.reshape(GATES, -1, NC)[:, :, ::-1].reshape(table.shape)
    table = jnp.where(lax.axis_index("c") == 0, table, swapped)
    return jnp.dot(probs, table, precision=lax.Precision.HIGHEST)


def row_source(rows):
    block = NXL * rows
    dest = lax.broadcasted_iota(jnp.int32, (NY * NZ * block, 1), 0)
    k, rest = dest // (NY * block), dest % (NY * block)
    y, q = rest // block, rest % block
    xl, row = q // rows, q % rows
    dy = (lax.axis_index("y") - y + NY) % NY
    dxl = (lax.axis_index("xl") + xl) % NXL
    z = (lax.axis_index("z") + k) % NZ
    return (dy * NZ + z) * 2 * block + dxl * rows + row


def dot(a, b):
    return jnp.dot(a, b, preferred_element_type=jnp.float32)


def expert(rows_ref, ups, downs, outs, hidden_ref):
    units = ups[0].shape[1]
    for at, up in enumerate(ups):
        hidden_ref[:, at * units : (at + 1) * units] = jnp.maximum(
            dot(rows_ref[...], up[...]), 0.0
        ).astype(jnp.bfloat16)
    chunk, width = outs[0].shape
    step = width // 2
    for column in range(0, width, step):
        now = pl.ds(column, step)
        value = dot(hidden_ref[:, :units], downs[0][:, now]) + dot(
            hidden_ref[:, units:], downs[1][:, now]
        )
        for k, out in enumerate(outs):
            out[:, now] = value[k * chunk : (k + 1) * chunk].astype(out.dtype)


def own_kernel(source_ref, *refs):
    pieces, ups, downs = refs[:NY], refs[NY : NY + 2], refs[NY + 2 : NY + 4]
    outs, rows_ref, every_ref, hidden_ref = refs[NY + 4 : -3], *refs[-3:]
    piece_rows, half = pieces[0].shape
    for dy, piece in enumerate(pieces):
        every_ref[dy * piece_rows : (dy + 1) * piece_rows, :] = piece[...]
    shape = (source_ref.shape[0], every_ref.shape[0])
    columns = lax.broadcasted_iota(jnp.int32, shape, 1)
    block = piece_rows // NZ // 2
    for q in range(2):
        order = jnp.where(columns == source_ref[...] + q * block, 1.0, 0.0).astype(jnp.bfloat16)
        rows_ref[:, q * half : (q + 1) * half] = dot(order, every_ref[...]).astype(jnp.bfloat16)
    expert(rows_ref, ups, downs, outs, hidden_ref)


def other_kernel(rows_ref, *refs):
    expert(rows_ref, refs[:2], refs[2:4], refs[4:-1], refs[-1])


def pack_kernel(*refs):
    out_ref = refs[-1]
    owners, _, half = out_ref.shape
    rows = out_ref.shape[1] // 4
    for j in range(2):
        own, ahead, behind = refs[3 * j : 3 * j + 3]
        total = own[...] + ahead[...].astype(jnp.float32) + behind[...].astype(jnp.float32)
        for owner in range(owners):
            for q in range(2):
                at = (2 * j + q) * rows
                out_ref[owner, at : at + rows, :] = total[
                    owner * rows : (owner + 1) * rows, q * half : (q + 1) * half
                ].astype(jnp.bfloat16)


def mix_kernel(mixing_ref, moved_ref, out_ref):
    pairs, _, half = moved_ref.shape
    outs, rows, _ = out_ref.shape
    for q in range(2):
        totals = [jnp.zeros((rows, half), jnp.float32) for _ in range(outs)]
        for pair in range(pairs):
            for j in range(2):
                at = (2 * j + q) * rows
                value = moved_ref[pair, at : at + rows, :].astype(jnp.float32)
                for k in range(outs):
                    column = k * 2 * pairs + 2 * pair + j
                    totals[k] = totals[k] + mixing_ref[:, column : column + 1] * value
        for k in range(outs):
            out_ref[k, :, q * half : (q + 1) * half] = totals[k].astype(jnp.bfloat16)


def call(kernel, outs, scratch, flops, *args):
    vmem = pl.BlockSpec(memory_space=pltpu.VMEM)
    outs = [jax.ShapeDtypeStruct(*o) for o in outs]
    moved = sum(a.size * a.dtype.itemsize for a in (*args, *outs))
    return pl.pallas_call(
        kernel,
        out_shape=outs,
        in_specs=[vmem] * len(args),
        out_specs=[vmem] * len(outs),
        scratch_shapes=[pltpu.VMEM(*x) for x in scratch],
        cost_estimate=pl.CostEstimate(flops=flops, bytes_accessed=moved, transcendentals=0),
    )(*args)


def named(x, axis, by=1):
    return shift(x, axis, by)


def sum_along_z(parts, ahead, behind):
    up = parts[ahead]
    for k in range(ahead - 1, -1, -1):
        up = named(up, "z", 1)
        if k:
            up = (up.astype(jnp.float32) + parts[k]).astype(jnp.bfloat16)
    down = parts[NZ - behind]
    for k in range(NZ - behind + 1, NZ + 1):
        down = named(down, "z", -1)
        if k < NZ:
            down = (down.astype(jnp.float32) + parts[k]).astype(jnp.bfloat16)
    return parts[0], up, down


def on_device(samples, gate_weight, up_weight, down_weight):
    rows, width = samples.shape
    up, down = up_weight[0], down_weight[0]
    units = up.shape[1]
    half = width // 2
    block = NXL * rows
    total = NY * NZ * block
    chunk = total // NZ

    beside = named(samples, "xl")
    far_up, far_down = named(up, "xh"), named(down, "xh")
    other_up, other_down = named(up, "c"), named(down, "c")
    blocks = jnp.concatenate(
        [x[:, q * half : (q + 1) * half] for q in range(2) for x in (samples, beside)], axis=0
    )
    same = jnp.broadcast_to(blocks[None], (NZ, 2 * block, half))
    near = lax.all_to_all(same, "z", split_axis=0, concat_axis=0, tiled=True)
    near = near.reshape(NZ * 2 * block, half)
    pieces = [near] + [named(near, "y", dy) for dy in range(1, NY)]
    both_up, both_down = named(far_up, "c"), named(far_down, "c")

    limits = ((4, 3), (3, 4))
    types = [
        [jnp.bfloat16 if k in (ahead, NZ - behind) else jnp.float32 for k in range(NZ)]
        for ahead, behind in limits
    ]
    outs = [[((chunk, width), t) for t in ts] for ts in types]
    flops = 8 * total * units * width
    ordered = ((total, width), jnp.bfloat16)
    *own_parts, ordered_rows = call(
        own_kernel, [*outs[0], ordered],
        [((2 * total, half), jnp.bfloat16), ((total, 2 * units), jnp.bfloat16)],
        flops + 8 * total * total * half,
        row_source(rows), *pieces, up, far_up, down, far_down,
    )
    other_parts = call(
        other_kernel, outs[1], [((total, 2 * units), jnp.bfloat16)], flops,
        ordered_rows, other_up, both_up, other_down, both_down,
    )
    summed = []
    for at, parts in enumerate((own_parts, other_parts)):
        summed.extend(sum_along_z(parts, *limits[at]))
    (packed,) = call(pack_kernel, [((NY * NXL, 4 * rows, half), jnp.bfloat16)], [], 4 * chunk * width, *summed)
    moved = lax.all_to_all(packed, ("y", "xl"), split_axis=0, concat_axis=0, tiled=True)
    mixing = gate_mix(samples, gate_weight)
    (out,) = call(
        mix_kernel, [((TASKS + 1, rows, width), jnp.bfloat16)], [],
        2 * rows * 5 * EXPERTS * width, mixing, moved,
    )
    return out.transpose(1, 0, 2)


def solution(mesh):
    torus = Mesh(mesh.devices.reshape(SIZES), AXES)
    ex, tp = AXES[:3], AXES[3:]
    return jax.shard_map(
        on_device,
        mesh=torus,
        in_specs=(P(AXES, None), P(), P(ex, None, tp), P(ex, tp, None)),
        out_specs=P(AXES, None, None),
        check_vma=False,
    )
```
